32 devices in a mesh: blk: 4 (over x, core), grp: 8 (over z, y).
Axes of the slice: x: 2, y: 2, z: 4, core: 2. Of those that a mesh axis runs over, the one named last changes fastest.
Arguments:
- design: float32 [8, 4096], P(None, ('blk', 'grp')), may hold values from -5 to 5
- lengthscales: float32 [8], replicated, may hold values from 0.55 to 0.85
- counts: int32 [4096], P(('blk', 'grp')), may hold values from 1 to 16
- noise_base: float32 [1], replicated, may hold values from 0.5 to 2
- targets: float32 [16, 4096], P(None, ('blk', 'grp')), may hold values from -6 to 6
Outputs:
- solution: float32 [16, 4096], P(None, ('blk', 'grp'))
- residual: float32 [16, 4096], P(None, ('blk', 'grp'))
- image: float32 [16, 4096], P(None, ('blk', 'grp'))
The draws below stay inside these ranges and needn't reach their ends.
All inputs are finite; a program needn't handle non-finite values.
Results may differ from the reference program's by a relative error of at most 0.0003.
Values sent between devices are 32-bit elements; how exact they have to be, the bound alone decides.
No kernel may reach another device: no remote copies, remote signals or barrier semaphores. Data moves between devices by JAX's collectives and lax.ppermute only.
A program may use at most 64 MiB of HBM per device.

```python
import math
import jax
import jax.numpy as jnp
from jax import lax

DIM = 8
NRHS = 16
N = 4096


def place_ends(array, own_key, smallest, top_value):
    place = [jax.random.randint(jax.random.fold_in(own_key, axis), (), 0, length) for axis, length in enumerate(array.shape)]
    widest = array.shape.index(max(array.shape))
    neighbour = place[:widest] + [(place[widest] + 1) % array.shape[widest]] + place[widest + 1:]
    return array.at[tuple(place)].set(smallest).at[tuple(neighbour)].set(top_value)


def shard_levels(rng, extent, split, low, high):
    def one(dim, blocks):
        steps = jax.random.uniform(jax.random.fold_in(jax.random.fold_in(rng, 6), dim), (blocks,), jnp.float32, low / len(split), high / len(split))
        return jnp.repeat(jnp.exp(steps), extent[dim] // blocks).reshape((-1,) + (1,) * (len(extent) - dim - 1))

    loudness = one(*split[0])
    for cut in split[1:]:
        loudness = loudness * one(*cut)
    return loudness


def gaussian(own_key, shape, spread, bound, shards=(), kind=jnp.bfloat16):
    result = jax.random.normal(own_key, shape, jnp.float32) * spread
    if len(shards) > 0:
        result = shard_levels(own_key, shape, shards, -0.22, 0.18) * result
    return jnp.clip(result, min=-bound, max=bound).astype(kind)


def setup_inputs(seed: int = 0) -> dict:
    seeds = jax.random.split(jax.random.key(seed), 6)
    return {
        "design": gaussian(seeds[0], (DIM, N), 1.0, 5.0, ((1, 32),), jnp.float32),
        "lengthscales": jnp.clip(jnp.exp(jax.random.uniform(seeds[1], (DIM,), jnp.float32, math.log(0.55), math.log(0.85))), 0.55, 0.85),
        "counts": place_ends(jax.random.randint(seeds[2], (N,), 1, 17), jax.random.fold_in(seeds[2], 1), 1, 16).astype(jnp.int32),
        "noise_base": jnp.clip(jnp.exp(jax.random.uniform(seeds[3], (1,), jnp.float32, math.log(0.5), math.log(2.0))), 0.5, 2.0),
        "targets": gaussian(seeds[4], (NRHS, N), 1.0, 6.0, ((1, 32),), jnp.float32),
    }


ROOT_FIVE = 2.23606797749979

def kernel_terms(own_scaled, own_square, col_scaled, col_dirs, running):
    columns = col_scaled.shape[1]
    block_width = math.gcd(columns, 2048)
    block_count = columns // block_width

    def advance(block_index, partial_sum):
        offset = block_index * block_width
        chosen = lax.dynamic_slice_in_dim(col_scaled, offset, block_width, 1)
        chosen_dirs = lax.dynamic_slice_in_dim(col_dirs, offset, block_width, 1)
        chosen_square = lax.optimization_barrier(jnp.sum(chosen * chosen, 0))
        inner_products = jnp.einsum('dr,dc->rc', own_scaled, chosen, precision=lax.Precision.HIGHEST)
        dist_square = jnp.maximum(own_square[:, None] + chosen_square[None, :] - 2.0 * inner_products, 0.0)
        radius = jnp.sqrt(dist_square)
        kernel_tile = (1.0 + ROOT_FIVE * radius + 5.0 / 3.0 * dist_square) * jnp.exp(-ROOT_FIVE * radius)
        return partial_sum + jnp.einsum('kc,rc->kr', chosen_dirs, kernel_tile, precision=lax.Precision.HIGHEST)
    return lax.fori_loop(0, block_count, advance, running)

def operator_apply(scaled, squares, noise_diag, direction):
    total_rows = scaled.shape[1]
    row_width = math.gcd(total_rows, 512)
    row_count = total_rows // row_width

    def one_block(block_index):
        offset = (block_index * row_width).astype(jnp.int32)
        own = lax.dynamic_slice_in_dim(scaled, offset, row_width, 1)
        own_sq = lax.dynamic_slice_in_dim(squares, offset, row_width, 0)
        zero_start = jnp.zeros((direction.shape[0], row_width), jnp.float32)
        return kernel_terms(own, own_sq, scaled, direction, zero_start)
    blocks = lax.map(one_block, jnp.arange(row_count, dtype=jnp.int32))
    product_sum = jnp.transpose(blocks, (1, 0, 2)).reshape(direction.shape)
    return product_sum + noise_diag[None, :] * direction

def reference(design, lengthscales, counts, noise_base, targets):
    scaled = design / lengthscales[:, None]
    squares = lax.optimization_barrier(jnp.sum(scaled * scaled, 0))
    noise_diag = noise_base[0] / counts.astype(jnp.float32)
    first = operator_apply(scaled, squares, noise_diag, targets)
    gammas = lax.optimization_barrier(jnp.sum(targets * targets, 1))
    deltas = lax.optimization_barrier(jnp.sum(first * targets, 1))
    further = operator_apply(scaled, squares, noise_diag, first)
    alphas = (gammas / deltas)[:, None]
    solution = alphas * targets
    residual = targets - alphas * first
    image = first - alphas * further
    return (solution, residual, image)
```

```python
import functools

import jax
import jax.numpy as jnp
from jax import lax
from jax.experimental import pallas as pl
from jax.experimental.pallas import tpu as pltpu
from jax.sharding import PartitionSpec as P

ROOT_FIVE = 2.23606797749979
AXES = ("blk", "grp")
TINY = 1e-30


def split3(x):
    high = x.astype(jnp.bfloat16)
    rest = x - high.astype(jnp.float32)
    middle = rest.astype(jnp.bfloat16)
    low = (rest - middle.astype(jnp.float32)).astype(jnp.bfloat16)
    return high, middle, low


def split2(x):
    high = x.astype(jnp.bfloat16)
    return high, (x - high.astype(jnp.float32)).astype(jnp.bfloat16)


def augment(points, own):
    high, middle, low = split3(points)
    squares = jnp.sum(points * points, 0, keepdims=True)
    sq = split3(jnp.broadcast_to(squares, points.shape))
    one = jnp.ones(points.shape, jnp.bfloat16)
    row = lax.broadcasted_iota(jnp.int32, points.shape, 0)

    def pick(parts):
        a, b, c = (part.astype(jnp.float32) for part in parts)
        zero = jnp.zeros(points.shape, jnp.float32)
        return jnp.where(row == 0, a, jnp.where(row == 1, b, jnp.where(row == 2, c, zero))).astype(jnp.bfloat16)

    if own:
        high, middle, low = (part * jnp.bfloat16(-2.0) for part in (high, middle, low))
        parts = [high, high, middle, high, low, middle, pick(sq), one]
    else:
        parts = [high, middle, high, low, high, middle, one, pick(sq)]
    return jnp.concatenate(parts, 0)


def matern(dist):
    dist = jnp.maximum(dist, TINY)
    radius = ROOT_FIVE * (dist * lax.rsqrt(dist))
    return (1.0 + radius + (5.0 / 3.0) * dist) * jnp.exp(-radius)


def dot_nt(a, b):
    return lax.dot_general(a, b, (((1,), (1,)), ((), ())), preferred_element_type=jnp.float32)


def dot_tn(a, b):
    return lax.dot_general(a, b, (((0,), (0,)), ((), ())), preferred_element_type=jnp.float32)


def first_kernel(dim, width, own_ref, scale_ref, noise_ref, all_ref, first_ref, high_ref, low_ref):
    blocks = all_ref.shape[0]
    columns = all_ref.shape[2]
    rhs = all_ref.shape[1] - dim
    scale = scale_ref[...]
    own = augment(own_ref[0:dim, :] / scale, True)
    total = jnp.zeros((own_ref.shape[1], 2 * rhs), jnp.float32)
    for start in range(0, blocks, width):
        points = jnp.concatenate([all_ref[start + k, 0:dim, :] for k in range(width)], 1)
        vectors = jnp.concatenate([all_ref[start + k, dim:, :] for k in range(width)], 1)
        tile = matern(dot_tn(own, augment(points / scale, False)))
        high, low = split2(tile)
        place = pl.ds(start * columns, width * columns)
        high_ref[:, place] = high
        low_ref[:, place] = low
        v_high, v_low = split2(vectors)
        total = total + dot_nt(high, jnp.concatenate([v_high, v_low], 0))
        total = total + dot_nt(low, jnp.concatenate([v_high, jnp.zeros_like(v_low)], 0))
    product = total[:, 0:rhs] + total[:, rhs:]
    first_ref[...] = product.T + noise_ref[...] * own_ref[dim:, :]


def last_kernel(dim, width, own_ref, first_ref, noise_ref, all_ref, firsts_ref, high_ref, low_ref,
                solution_ref, residual_ref, image_ref):
    blocks = all_ref.shape[0]
    columns = all_ref.shape[2]
    rhs = all_ref.shape[1] - dim
    total = jnp.zeros((high_ref.shape[0], 2 * rhs), jnp.float32)
    gammas = jnp.zeros((rhs, columns), jnp.float32)
    deltas = jnp.zeros((rhs, columns), jnp.float32)
    for start in range(0, blocks, width):
        for k in range(width):
            target = all_ref[start + k, dim:, :]
            gammas = gammas + target * target
            deltas = deltas + target * firsts_ref[start + k]
        vectors = jnp.concatenate([firsts_ref[start + k] for k in range(width)], 1)
        place = pl.ds(start * columns, width * columns)
        v_high, v_low = split2(vectors)
        total = total + dot_nt(high_ref[:, place], jnp.concatenate([v_high, v_low], 0))
        total = total + dot_nt(low_ref[:, place], jnp.concatenate([v_high, jnp.zeros_like(v_low)], 0))
    product = total[:, 0:rhs] + total[:, rhs:]
    first = first_ref[...]
    targets = own_ref[dim:, :]
    further = product.T + noise_ref[...] * first
    alphas = jnp.sum(gammas, 1, keepdims=True) / jnp.sum(deltas, 1, keepdims=True)
    solution_ref[...] = alphas * targets
    residual_ref[...] = targets - alphas * first
    image_ref[...] = first - alphas * further


def gather(x, size):
    return lax.all_to_all(jnp.broadcast_to(x[None], (size,) + x.shape), AXES, 0, 0)


def on_device(size, design, lengthscales, counts, noise_base, targets):
    dim, own = design.shape
    rhs = targets.shape[0]
    points = size * own
    noise = (noise_base[0] / counts.astype(jnp.float32))[None, :]
    packed = jnp.concatenate([design, targets], 0)
    everything = gather(packed, size)
    width = 4
    first, high, low = pl.pallas_call(
        functools.partial(first_kernel, dim, width),
        out_shape=(
            jax.ShapeDtypeStruct((rhs, own), jnp.float32),
            jax.ShapeDtypeStruct((own, points), jnp.bfloat16),
            jax.ShapeDtypeStruct((own, points), jnp.bfloat16),
        ),
        name="first_apply",
    )(packed, lengthscales[:, None], noise, everything)
    firsts = gather(first, size)
    shape = jax.ShapeDtypeStruct((rhs, own), jnp.float32)
    return pl.pallas_call(
        functools.partial(last_kernel, dim, width),
        out_shape=(shape, shape, shape),
        name="second_apply",
    )(packed, first, noise, everything, firsts, high, low)


def solution(mesh):
    size = mesh.shape["blk"] * mesh.shape["grp"]
    in_specs = (P(None, AXES), P(), P(AXES), P(), P(None, AXES))
    out_specs = (P(None, AXES), P(None, AXES), P(None, AXES))
    return jax.shard_map(
        functools.partial(on_device, size), mesh=mesh, in_specs=in_specs, out_specs=out_specs, check_vma=False
    )
```

```python
import functools
import math

import jax
import jax.numpy as jnp
from jax import lax
from jax.experimental import pallas as pl
from jax.experimental.pallas import tpu as pltpu
from jax.sharding import PartitionSpec as P

ROOT_FIVE = 2.23606797749979
LN_TWO = math.log(2.0)
AXES = ("blk", "grp")
TINY = 1e-30
PARAMS = pltpu.CompilerParams(vmem_limit_bytes=32 << 20)
VMEM = pl.BlockSpec(memory_space=pltpu.VMEM)
SMEM = pl.BlockSpec(memory_space=pltpu.SMEM)
FAST = jnp.bfloat16


def split3(x):
    high = x.astype(FAST)
    rest = x - high.astype(jnp.float32)
    middle = rest.astype(FAST)
    low = (rest - middle.astype(jnp.float32)).astype(FAST)
    return high, middle, low


def split2(x):
    high = x.astype(FAST)
    return high, (x - high.astype(jnp.float32)).astype(FAST)


def augment(points, own):
    parts = split3(points)
    squares = jnp.sum(points * points, 0, keepdims=True)
    row = lax.broadcasted_iota(jnp.int32, points.shape, 0)
    a, b, c = (part.astype(jnp.float32) for part in split3(jnp.broadcast_to(squares, points.shape)))
    zero = jnp.zeros(points.shape, jnp.float32)
    one = jnp.ones(points.shape, jnp.float32)
    three = jnp.where(row == 0, a, jnp.where(row == 1, b, jnp.where(row == 2, c, zero))).astype(FAST)
    ones = jnp.where(row < 3, one, zero).astype(FAST)
    if own:
        high, middle, low = (part * FAST(-2.0) for part in parts)
        rows = [high, high, middle, high, low, middle, three, ones]
    else:
        high, middle, low = parts
        rows = [high, middle, high, low, high, middle, ones, three]
    return jnp.concatenate(rows, 0)


def matern(dist):
    dist = jnp.maximum(dist, TINY)
    radius = dist * lax.rsqrt(dist)
    return (1.0 + LN_TWO * radius + (LN_TWO * LN_TWO / 3.0) * dist) * jnp.exp2(-radius)


def dot_nt(a, b):
    return lax.dot_general(a, b, (((1,), (1,)), ((), ())), preferred_element_type=jnp.float32)


def dot_nn(a, b):
    return lax.dot_general(a, b, (((1,), (0,)), ((), ())), preferred_element_type=jnp.float32)


def lanes(blocks):
    return blocks[0] if len(blocks) == 1 else jnp.concatenate(blocks, 1)


def pack_kernel(scale_ref, base_ref, design_ref, counts_ref, targets_ref, packed_ref):
    dim = design_ref.shape[0]
    rhs = targets_ref.shape[0]
    row = lax.broadcasted_iota(jnp.int32, design_ref.shape, 0)
    scale = jnp.full(design_ref.shape, scale_ref[0], jnp.float32)
    for d in range(1, dim):
        scale = jnp.where(row == d, scale_ref[d], scale)
    packed_ref[0:dim, :] = (design_ref[...] / scale) * (ROOT_FIVE / LN_TWO)
    packed_ref[dim : dim + rhs, :] = targets_ref[...]
    noise = base_ref[0] / counts_ref[...].astype(jnp.float32)
    packed_ref[dim + rhs :, :] = jnp.broadcast_to(noise, (packed_ref.shape[0] - dim - rhs, noise.shape[1]))


def add_columns(dim, own, stack_ref, total, kept, where):
    count = stack_ref.shape[0]
    step = 2 if count % 2 == 0 else 1
    for start in range(0, count, step):
        points = lanes([stack_ref[start + k, 0:dim, :] for k in range(step)])
        vectors = lanes([stack_ref[start + k, dim:, :] for k in range(step)])
        high, low = split2(matern(dot_nn(own, augment(points, False))))
        if start == 0:
            size = stack_ref.shape[2]
            kept[0][:, pl.ds(where * size, size)] = high[:, 0:size]
            kept[1][:, pl.ds(where * size, size)] = low[:, 0:size]
        v_high, v_low = split2(vectors)
        total = total + dot_nt(high, jnp.concatenate([v_high, v_low], 0))
        total = total + dot_nt(low, jnp.concatenate([v_high, jnp.zeros_like(v_low)], 0))
    return total


def start_kernel(dim, count, *refs):
    line_ref = refs[0]
    stacks = refs[0:count]
    own_ref, total_ref, high_ref, low_ref = refs[count:]
    points = lanes([line_ref[k, 0:dim, :] for k in range(line_ref.shape[0])])
    own = augment(points, True).astype(jnp.float32).T.astype(FAST)
    own_ref[...] = own
    total = jnp.zeros(total_ref.shape, jnp.float32)
    for place, stack in enumerate(stacks):
        total = add_columns(dim, own, stack, total, (high_ref, low_ref), place)
    total_ref[...] = total


def more_kernel(dim, count, own_ref, before_ref, *refs):
    stacks = refs[0:count]
    total_ref, high_ref, low_ref = refs[count:]
    own = own_ref[...]
    total = before_ref[...]
    for place, stack in enumerate(stacks):
        total = add_columns(dim, own, stack, total, (high_ref, low_ref), place)
    total_ref[...] = total


def close_kernel(dim, count, plan, own_ref, before_ref, line_ref, noise_ref, *refs):
    stacks = refs[0:count]
    earlier = len(set(source for source, _ in plan)) - 1
    kept = refs[count : count + 2 * earlier]
    first_ref, parts_ref, high_ref, low_ref = refs[count + 2 * earlier :]
    own = own_ref[...]
    total = before_ref[...]
    for place, stack in enumerate(stacks):
        total = add_columns(dim, own, stack, total, (high_ref, low_ref), place)
    blocks = line_ref.shape[0]
    size = line_ref.shape[2]
    rhs = line_ref.shape[1] - dim
    product = total.T
    targets = lanes([line_ref[k, dim:, :] for k in range(blocks)])
    noise = lanes([noise_ref[k, 0:1, :] for k in range(blocks)])
    first = product[0:rhs, :] + product[rhs:, :] + noise * targets
    first_ref[...] = first[:, 0:size]
    gammas = jnp.sum(targets * targets, 1, keepdims=True)
    deltas = jnp.sum(first * targets, 1, keepdims=True)
    lane = lax.broadcasted_iota(jnp.int32, (rhs, size), 1)
    sums = jnp.where(lane == 0, gammas, jnp.where(lane == 1, deltas, 0.0))
    f_high, f_low = split2(first)
    both = jnp.concatenate([f_high, f_low], 0)
    pairs = [(kept[2 * k], kept[2 * k + 1]) for k in range(earlier)] + [(high_ref, low_ref)]
    for mask, (source, place) in enumerate(plan):
        at = pl.ds(place * size, size)
        part = dot_nn(both, pairs[source][0][:, at])
        parts_ref[mask, 0:rhs, :] = part[0:rhs, :] + part[rhs:, :] + dot_nn(f_high, pairs[source][1][:, at])
        parts_ref[mask, rhs:, :] = sums


def end_kernel(dim, count, packed_ref, first_ref, *refs):
    parts = refs[0:count]
    solution_ref, residual_ref, image_ref = refs[count:]
    rhs = first_ref.shape[0]
    total = sum((part[...] for part in parts[1:]), parts[0][...])
    first = first_ref[...]
    targets = packed_ref[dim : dim + rhs, :]
    noise = packed_ref[dim + rhs : dim + rhs + 1, :]
    further = total[0:rhs, :] + noise * first
    alphas = total[rhs:, 0:1] / total[rhs:, 1:2]
    solution_ref[...] = alphas * targets
    residual_ref[...] = targets - alphas * first
    image_ref[...] = first - alphas * further


def call(body, operands, specs, shapes, name, flops, scratch=()):
    return pl.pallas_call(
        body,
        in_specs=specs,
        out_specs=tuple(VMEM for _ in shapes),
        out_shape=tuple(jax.ShapeDtypeStruct(shape, dtype) for shape, dtype in shapes),
        scratch_shapes=scratch,
        compiler_params=PARAMS,
        cost_estimate=pl.CostEstimate(flops=flops, transcendentals=0, bytes_accessed=0),
        name=name,
    )(*operands)


def on_device(blk, grp, design, lengthscales, counts, noise_base, targets):
    dim, size = design.shape
    rhs = targets.shape[0]
    devices = blk * grp
    core = math.gcd(blk, 2)
    line = math.gcd(grp, 4)
    rest = grp // line
    line_masks = [k * rest for k in range(line)]
    plane_masks = [b * core * grp + r for b in range(blk // core) for r in range(rest)]

    def swap(value, mask):
        return lax.ppermute(value, AXES, [(i, i ^ mask) for i in range(devices)])

    f32 = jnp.float32
    packed = call(
        pack_kernel,
        (lengthscales, noise_base, design, counts[None, :], targets),
        [SMEM, SMEM, VMEM, VMEM, VMEM],
        [((dim + rhs + 8, size), f32)],
        "pack",
        1,
    )[0]
    blocks = jnp.stack([packed] + [swap(packed, mask) for mask in line_masks[1:]])
    near = blocks[:, 0 : dim + rhs, :]
    noise = blocks[:, dim + rhs :, :]
    there = [swap(near, mask) for mask in plane_masks[1:]]
    rows = line * size
    work = 2 * 80 * rows * rows

    def kept(count):
        return [((rows, count * size), FAST), ((rows, count * size), FAST)]

    if core == 2:
        opening = [near, swap(near, grp)]
        middle = there
        last = [swap(value, grp) for value in there]
    else:
        opening, middle, last = [near], [], there
    own, total, *saved = call(
        functools.partial(start_kernel, dim, len(opening)),
        opening,
        [VMEM] * len(opening),
        [((rows, 64), FAST), ((rows, 2 * rhs), f32)] + kept(len(opening)),
        "columns_a",
        work * len(opening),
    )
    plan = [(0, 0)]
    source = 0
    if middle:
        source += 1
        total, *extra = call(
            functools.partial(more_kernel, dim, len(middle)),
            [own, total] + middle,
            [VMEM] * (2 + len(middle)),
            [((rows, 2 * rhs), f32)] + kept(len(middle)),
            "columns_b",
            work * len(middle),
        )
        saved += extra
        plan += [(source, k) for k in range(len(middle))]
    source += 1
    if core == 2:
        plan.append((0, 1))
    plan += [(source, k) for k in range(len(last))]
    first, parts = call(
        functools.partial(close_kernel, dim, len(last), plan),
        [own, total, near, noise] + last + saved,
        [VMEM] * (4 + len(last) + len(saved)),
        [((rhs, size), f32), ((len(plan), 2 * rhs, size), f32)],
        "columns_c",
        work * len(last),
        scratch=[pltpu.VMEM(shape, dtype) for shape, dtype in kept(max(1, len(last)))],
    )
    half = len(plan) // core
    if core == 2:
        parts = parts[0:half] + swap(parts[half:], grp)
    pieces = [parts[0]] + [swap(parts[k], plane_masks[k]) for k in range(1, half)]
    return call(
        functools.partial(end_kernel, dim, len(pieces)),
        [packed, first] + pieces,
        [VMEM] * (2 + len(pieces)),
        [((rhs, size), f32)] * 3,
        "finish",
        1,
    )


def solution(mesh):
    in_specs = (P(None, AXES), P(), P(AXES), P(), P(None, AXES))
    out_specs = (P(None, AXES), P(None, AXES), P(None, AXES))
    body = functools.partial(on_device, mesh.shape["blk"], mesh.shape["grp"])
    return jax.shard_map(body, mesh=mesh, in_specs=in_specs, out_specs=out_specs, check_vma=False)
```

```python
import functools
import math

import jax
import jax.numpy as jnp
from jax import lax
from jax.experimental import pallas as pl
from jax.experimental.pallas import tpu as pltpu
from jax.sharding import PartitionSpec as P


ROOT_FIVE = 2.23606797749979
LN_TWO = math.log(2.0)
AXES = ("blk", "grp")
TINY = 1e-30
PARAMS = pltpu.CompilerParams(vmem_limit_bytes=32 << 20)
VMEM = pl.BlockSpec(memory_space=pltpu.VMEM)
FAST = jnp.bfloat16


def split3(x):
    high = x.astype(FAST)
    rest = x - high.astype(jnp.float32)
    middle = rest.astype(FAST)
    low = (rest - middle.astype(jnp.float32)).astype(FAST)
    return high, middle, low


def split2(x):
    high = x.astype(FAST)
    return high, (x - high.astype(jnp.float32)).astype(FAST)


def augment(points, own):
    parts = split3(points)
    squares = jnp.sum(points * points, 0, keepdims=True)
    row = lax.broadcasted_iota(jnp.int32, points.shape, 0)
    a, b, c = (part.astype(jnp.float32) for part in split3(jnp.broadcast_to(squares, points.shape)))
    zero = jnp.zeros(points.shape, jnp.float32)
    one = jnp.ones(points.shape, jnp.float32)
    three = jnp.where(row == 0, a, jnp.where(row == 1, b, jnp.where(row == 2, c, zero))).astype(FAST)
    ones = jnp.where(row < 3, one, zero).astype(FAST)
    if own:
        high, middle, low = (part * FAST(-2.0) for part in parts)
        rows = [high, high, middle, high, low, middle, three, ones]
    else:
        high, middle, low = parts
        rows = [high, middle, high, low, high, middle, ones, three]
    return jnp.concatenate(rows, 0)


def matern(dist):
    dist = jnp.maximum(dist, TINY)
    radius = dist * lax.rsqrt(dist)
    return ((LN_TWO / 3.0) * dist + 1.0 / LN_TWO + radius) * jnp.exp2(-radius)


def dot(a, b, over_a, over_b):
    return lax.dot_general(a, b, (((over_a,), (over_b,)), ((), ())), preferred_element_type=jnp.float32)


def lanes(blocks):
    return blocks[0] if len(blocks) == 1 else jnp.concatenate(blocks, 1)


def scaled(points, scale):
    return points / jnp.tile(scale, (1, points.shape[1] // scale.shape[1])) * (ROOT_FIVE / LN_TWO)


def add_columns(dim, own, scale, stack_ref, total, kept, where):
    count, _, size = stack_ref.shape
    points = lanes([stack_ref[k, 0:dim, :] for k in range(count)])
    vectors = lanes([stack_ref[k, dim:, :] for k in range(count)])
    high, low = split2(matern(dot(augment(scaled(points, scale), False), own, 0, 0)))
    at = pl.ds(where * count * size, count * size)
    kept[0][at, :] = high
    kept[1][at, :] = low
    v_high, v_low = split2(vectors)
    total = total + dot(jnp.concatenate([v_high, v_low], 0), high, 1, 0)
    return total + dot(jnp.concatenate([v_high, jnp.zeros_like(v_low)], 0), low, 1, 0)


def columns_kernel(dim, count, opening, final, settings_ref, packed_ref, *refs):
    scale = settings_ref[0:dim, :]
    if opening:
        rows, refs = refs[0:opening], refs[opening:]
        own = augment(scaled(lanes([row[0:dim, :] for row in rows]), scale), True)
    else:
        own, before, refs = refs[0][...], refs[1][...], refs[2:]
    stacks, outs = refs[0:count], refs[count:]
    rhs = packed_ref.shape[0] - dim
    total = jnp.zeros((2 * rhs, own.shape[1]), jnp.float32) if opening else before
    for place, stack in enumerate(stacks):
        total = add_columns(dim, own, scale, stack, total, outs[-2:], place)
    if opening and not final:
        outs[0][...] = own
    if final:
        sums_ref = outs[0]
        blocks, _, size = sums_ref.shape
        for k in range(blocks):
            at = slice(k * size, (k + 1) * size)
            part = LN_TWO * (total[0:rhs, at] + total[rhs:, at])
            if k == 0:
                part = part + settings_ref[dim : dim + 1, :] * packed_ref[dim:, :]
            sums_ref[k] = part
    else:
        outs[-3][...] = total


def close_kernel(dim, plan, place_of, *refs):
    first_ref, parts_ref = refs[-2:]
    shares, parts = plan[0]
    rows, sums, kept = refs[0:shares], refs[shares : shares + parts], refs[shares + parts : -2]
    rhs, size = first_ref.shape
    targets = lanes([row[dim:, :] for row in rows])
    first = lanes([sum((sums[m][k ^ m] for m in range(1, parts)), sums[0][k]) for k in range(shares)])
    first_ref[...] = first[:, 0:size]
    gammas = jnp.sum(targets * targets, 1, keepdims=True)
    deltas = jnp.sum(first * targets, 1, keepdims=True)
    lane = lax.broadcasted_iota(jnp.int32, (8, size), 1)
    pairs = jnp.zeros((8, size), jnp.float32)
    for k in range(rhs // 8):
        pairs = jnp.where(lane == 2 * k, gammas[8 * k : 8 * k + 8], pairs)
        pairs = jnp.where(lane == 2 * k + 1, deltas[8 * k : 8 * k + 8], pairs)
    f_high, f_low = split2(LN_TWO * first)
    both = jnp.concatenate([f_high, f_low], 0)
    here = place_of()
    masks = iter(plan[1])
    for source in range(0, len(kept), 2):
        part = dot(both, kept[source][...], 1, 1)
        part = part[0:rhs, :] + part[rhs:, :] + dot(f_high, kept[source + 1][...], 1, 1)
        for k in range(part.shape[1] // size):
            to = here ^ next(masks)
            parts_ref[to, 0:rhs, :] = part[:, k * size : (k + 1) * size]
            parts_ref[to, rhs:, :] = pairs


def end_kernel(dim, settings_ref, packed_ref, first_ref, parts_ref, solution_ref, residual_ref, image_ref):
    rhs = first_ref.shape[0]
    total = sum((parts_ref[k] for k in range(1, parts_ref.shape[0])), parts_ref[0])
    first = first_ref[...]
    targets = packed_ref[dim:, :]
    further = total[0:rhs, :] + settings_ref[dim : dim + 1, :] * first
    gammas = jnp.concatenate([total[rhs:, 2 * k : 2 * k + 1] for k in range(rhs // 8)], 0)
    deltas = jnp.concatenate([total[rhs:, 2 * k + 1 : 2 * k + 2] for k in range(rhs // 8)], 0)
    alphas = gammas / deltas
    solution_ref[...] = alphas * targets
    residual_ref[...] = targets - alphas * first
    image_ref[...] = first - alphas * further


def call(body, operands, shapes, flops):
    return pl.pallas_call(
        body,
        in_specs=[VMEM] * len(operands),
        out_specs=tuple(VMEM for _ in shapes),
        out_shape=tuple(jax.ShapeDtypeStruct(shape, dtype) for shape, dtype in shapes),
        compiler_params=PARAMS,
        cost_estimate=pl.CostEstimate(flops=flops, transcendentals=0, bytes_accessed=0),
    )(*operands)


def layout(blk, grp):
    core = math.gcd(blk, 2)
    line = math.gcd(grp, 4)
    far = math.gcd(line, 2)
    rest = grp // line
    part = grp // far
    plane = [b * core * grp + r for b in range(blk // core) for r in range(rest)]
    return core, line // far, far, rest, part, plane


def on_device(blk, grp, design, lengthscales, counts, noise_base, targets):
    dim, size = design.shape
    rhs = targets.shape[0]
    devices = blk * grp
    core, near, far, rest, part, plane = layout(blk, grp)

    def swap(value, mask):
        return lax.ppermute(value, AXES, [(i, i ^ mask) for i in range(devices)])

    f32 = jnp.float32
    settings = jnp.concatenate([
        jnp.broadcast_to(lengthscales[:, None], (dim, size)),
        jnp.broadcast_to((noise_base[0] / counts.astype(f32))[None, :], (8, size)),
    ])
    packed = jnp.concatenate([design, targets])
    stack = [packed] + [swap(packed, k * rest) for k in range(1, near)]
    stack = jnp.stack(stack)
    stacks = [stack] + [swap(stack, mask) for mask in plane[1:]]
    rows = [packed]
    for steps, stride in ((far, part), (core, grp)):
        if steps == 2:
            rows += [swap(value, stride) for value in rows]
    shares = len(rows)
    points = shares * size
    third = -(-(len(stacks) - 1) // 3)
    groups = [stacks[0:1], stacks[1 : 1 + third], stacks[1 + third : 1 + 2 * third], stacks[1 + 2 * third :]]
    groups = [group for group in groups if group]
    kept = []
    own = total = None
    for number, group in enumerate(groups):
        final = number == len(groups) - 1
        shapes = [] if number or final else [((64, points), FAST)]
        shapes += [((shares, rhs, size), f32)] if final else [((2 * rhs, points), f32)]
        shapes += [((len(group) * near * size, points), FAST)] * 2
        found = call(
            functools.partial(columns_kernel, dim, len(group), 0 if number else shares, final),
            [settings, packed] + ([own, total] if number else rows) + group,
            shapes,
            200 * 80 * points * near * size * len(group),
        )
        *found, total, high, low = found
        own = found[0] if found else own
        kept += [high, low]
    turn = far
    if core == 2:
        total = total + jnp.roll(swap(total, grp), turn, 0)
    sums = [total] + ([swap(total, part)] if far == 2 else [])
    wide = near * rest
    columns = [mask // (core * grp) * wide + mask % grp + k * rest for mask in plane for k in range(near)]

    def place_of():
        return lax.axis_index("blk") // core * wide + lax.axis_index("grp") % wide

    members = blk // core * wide
    first, parts = call(
        functools.partial(close_kernel, dim, ((shares, len(sums)), columns), place_of),
        rows + sums + kept,
        [((rhs, size), f32), ((members, rhs + 8, size), f32)],
        200 * 80 * points * size,
    )
    teams = [
        [(b * core + c) * grp + f * part + r for b in range(blk // core) for r in range(part)]
        for c in range(core)
        for f in range(far)
    ]
    parts = lax.all_to_all(parts, AXES, 0, 0, axis_index_groups=teams)
    return call(functools.partial(end_kernel, dim), [settings, packed, first, parts], [((rhs, size), f32)] * 3, 1)


def solution(mesh):
    in_specs = (P(None, AXES), P(), P(AXES), P(), P(None, AXES))
    out_specs = (P(None, AXES), P(None, AXES), P(None, AXES))
    blk, grp = mesh.shape["blk"], mesh.shape["grp"]

    def body(*arguments):
        return on_device(blk, grp, *arguments)

    return jax.shard_map(body, mesh=mesh, in_specs=in_specs, out_specs=out_specs, check_vma=False)
```

```python
import functools
import math

import jax
import jax.numpy as jnp
from jax import lax
from jax.experimental import pallas as pl
from jax.experimental.pallas import tpu as pltpu
from jax.sharding import PartitionSpec as P


ROOT_FIVE = 2.23606797749979
LN_TWO = math.log(2.0)
AXES = ("blk", "grp")
TINY = 1e-30
PARAMS = pltpu.CompilerParams(vmem_limit_bytes=32 << 20)
VMEM = pl.BlockSpec(memory_space=pltpu.VMEM)
FAST = jnp.bfloat16


def split3(x):
    high = x.astype(FAST)
    rest = x - high.astype(jnp.float32)
    middle = rest.astype(FAST)
    low = (rest - middle.astype(jnp.float32)).astype(FAST)
    return high, middle, low


def split2(x):
    high = x.astype(FAST)
    return high, (x - high.astype(jnp.float32)).astype(FAST)


def augment(points, own):
    parts = split3(points)
    squares = jnp.sum(points * points, 0, keepdims=True)
    row = lax.broadcasted_iota(jnp.int32, points.shape, 0)
    a, b, c = (part.astype(jnp.float32) for part in split3(jnp.broadcast_to(squares, points.shape)))
    zero = jnp.zeros(points.shape, jnp.float32)
    one = jnp.ones(points.shape, jnp.float32)
    three = jnp.where(row == 0, a, jnp.where(row == 1, b, jnp.where(row == 2, c, zero))).astype(FAST)
    ones = jnp.where(row < 3, one, zero).astype(FAST)
    if own:
        high, middle, low = (part * FAST(-2.0) for part in parts)
        rows = [high, high, middle, high, low, middle, three, ones]
    else:
        high, middle, low = parts
        rows = [high, middle, high, low, high, middle, ones, three]
    return jnp.concatenate(rows, 0)


def matern(dist):
    dist = jnp.maximum(dist, TINY)
    radius = dist * lax.rsqrt(dist)
    return ((LN_TWO / 3.0) * dist + 1.0 / LN_TWO + radius) * jnp.exp2(-radius)


def dot(a, b, over_a, over_b):
    return lax.dot_general(a, b, (((over_a,), (over_b,)), ((), ())), preferred_element_type=jnp.float32)


def lanes(blocks):
    return blocks[0] if len(blocks) == 1 else jnp.concatenate(blocks, 1)


def scaled(points, scale):
    return points / jnp.tile(scale, (1, points.shape[1] // scale.shape[1])) * (ROOT_FIVE / LN_TWO)


def add_columns(dim, own, scale, stacks, total, kept, start):
    count, _, size = stacks[0].shape
    points = lanes([stack[k, 0:dim, :] for stack in stacks for k in range(count)])
    vectors = lanes([stack[k, dim:, :] for stack in stacks for k in range(count)])
    high, low = split2(matern(dot(augment(scaled(points, scale), False), own, 0, 0)))
    at = pl.ds(start * count * size, len(stacks) * count * size)
    kept[0][at, :] = high
    kept[1][at, :] = low
    v_high, v_low = split2(vectors)
    total = total + dot(jnp.concatenate([v_high, v_low], 0), high, 1, 0)
    return total + dot(jnp.concatenate([v_high, jnp.zeros_like(v_low)], 0), low, 1, 0)


def columns_kernel(dim, count, opening, final, settings_ref, *refs):
    scale = settings_ref[0:dim, :]
    if final:
        packed_ref, noise_ref, refs = refs[0], refs[1], refs[2:]
    if opening:
        rows, refs = refs[0:opening], refs[opening:]
        own = augment(scaled(lanes([row[0:dim, :] for row in rows]), scale), True)
    else:
        own, before, refs = refs[0][...], refs[1][...], refs[2:]
    stacks, outs = refs[0:count], refs[count:]
    rhs = stacks[0].shape[1] - dim
    total = jnp.zeros((2 * rhs, own.shape[1]), jnp.float32) if opening else before
    for start in range(0, count, 2):
        total = add_columns(dim, own, scale, stacks[start : start + 2], total, outs[-2:], start)
    if opening and not final:
        outs[0][...] = own
    if final:
        sums_ref = outs[0]
        blocks, _, size = sums_ref.shape
        for k in range(blocks):
            at = slice(k * size, (k + 1) * size)
            part = LN_TWO * (total[0:rhs, at] + total[rhs:, at])
            if k == 0:
                part = part + noise_ref[0:1, :] * packed_ref[dim:, :]
            sums_ref[k] = part
    else:
        outs[-3][...] = total


def close_kernel(dim, plan, place_of, *refs):
    first_ref, parts_ref = refs[-2:]
    shares, parts = plan[0]
    rows, sums, kept = refs[0:shares], refs[shares : shares + parts], refs[shares + parts : -2]
    rhs, size = first_ref.shape
    targets = lanes([row[dim:, :] for row in rows])
    first = lanes([sum((sums[m][k ^ m] for m in range(1, parts)), sums[0][k]) for k in range(shares)])
    first_ref[...] = first[:, 0:size]
    gammas = jnp.sum(targets * targets, 1, keepdims=True)
    deltas = jnp.sum(first * targets, 1, keepdims=True)
    lane = lax.broadcasted_iota(jnp.int32, (8, size), 1)
    pairs = jnp.zeros((8, size), jnp.float32)
    for k in range(rhs // 8):
        pairs = jnp.where(lane == 2 * k, gammas[8 * k : 8 * k + 8], pairs)
        pairs = jnp.where(lane == 2 * k + 1, deltas[8 * k : 8 * k + 8], pairs)
    f_high, f_low = split2(LN_TWO * first)
    both = jnp.concatenate([f_high, f_low], 0)
    here = place_of()
    masks = iter(plan[1])
    for source in range(0, len(kept), 2):
        part = dot(both, kept[source][...], 1, 1)
        part = part[0:rhs, :] + part[rhs:, :] + dot(f_high, kept[source + 1][...], 1, 1)
        for k in range(part.shape[1] // size):
            to = here ^ next(masks)
            parts_ref[to, 0:rhs, :] = part[:, k * size : (k + 1) * size]
            parts_ref[to, rhs:, :] = pairs


def end_kernel(dim, noise_ref, packed_ref, first_ref, parts_ref, solution_ref, residual_ref, image_ref):
    rhs = first_ref.shape[0]
    total = sum((parts_ref[k] for k in range(1, parts_ref.shape[0])), parts_ref[0])
    first = first_ref[...]
    targets = packed_ref[dim:, :]
    further = total[0:rhs, :] + noise_ref[0:1, :] * first
    gammas = jnp.concatenate([total[rhs:, 2 * k : 2 * k + 1] for k in range(rhs // 8)], 0)
    deltas = jnp.concatenate([total[rhs:, 2 * k + 1 : 2 * k + 2] for k in range(rhs // 8)], 0)
    alphas = gammas / deltas
    solution_ref[...] = alphas * targets
    residual_ref[...] = targets - alphas * first
    image_ref[...] = first - alphas * further


def call(body, operands, shapes, flops):
    return pl.pallas_call(
        body,
        in_specs=[VMEM] * len(operands),
        out_specs=tuple(VMEM for _ in shapes),
        out_shape=tuple(jax.ShapeDtypeStruct(shape, dtype) for shape, dtype in shapes),
        compiler_params=PARAMS,
        cost_estimate=pl.CostEstimate(flops=flops, transcendentals=0, bytes_accessed=0),
    )(*operands)


def layout(blk, grp):
    core = math.gcd(blk, 2)
    line = math.gcd(grp, 4)
    far = math.gcd(line, 2)
    rest = grp // line
    part = grp // far
    plane = [b * core * grp + r for b in range(blk // core) for r in range(rest)]
    return core, line // far, far, rest, part, plane


def on_device(blk, grp, design, lengthscales, counts, noise_base, targets):
    dim, size = design.shape
    rhs = targets.shape[0]
    devices = blk * grp
    core, near, far, rest, part, plane = layout(blk, grp)

    def swap(value, mask):
        return lax.ppermute(value, AXES, [(i, i ^ mask) for i in range(devices)])

    f32 = jnp.float32
    settings = jnp.broadcast_to(lengthscales[:, None], (dim, size))
    noise = jnp.broadcast_to((noise_base[0] / counts.astype(f32))[None, :], (8, size))
    packed = jnp.concatenate([design, targets])
    stack = [packed] + [swap(packed, k * rest) for k in range(1, near)]
    stack = jnp.stack(stack)
    stacks = [stack] + [swap(stack, mask) for mask in plane[1:]]
    rows = [packed]
    for steps, stride in ((far, part), (core, grp)):
        if steps == 2:
            rows += [swap(value, stride) for value in rows]
    shares = len(rows)
    points = shares * size
    half = -(-len(stacks) // 2)
    third = -(-3 * len(stacks) // 4)
    groups = [stacks[0:half], stacks[half:third], stacks[third:]]
    groups = [group for group in groups if group]
    kept = []
    own = total = None
    for number, group in enumerate(groups):
        final = number == len(groups) - 1
        shapes = [] if number or final else [((64, points), FAST)]
        shapes += [((shares, rhs, size), f32)] if final else [((2 * rhs, points), f32)]
        shapes += [((len(group) * near * size, points), FAST)] * 2
        found = call(
            functools.partial(columns_kernel, dim, len(group), 0 if number else shares, final),
            [settings] + ([packed, noise] if final else []) + ([own, total] if number else rows) + group,
            shapes,
            200 * 80 * points * near * size * len(group),
        )
        *found, total, high, low = found
        own = found[0] if found else own
        kept += [high, low]
    turn = far
    if core == 2:
        total = total + jnp.roll(swap(total, grp), turn, 0)
    sums = [total] + ([swap(total, part)] if far == 2 else [])
    wide = near * rest
    columns = [mask // (core * grp) * wide + mask % grp + k * rest for mask in plane for k in range(near)]

    def place_of():
        return lax.axis_index("blk") // core * wide + lax.axis_index("grp") % wide

    members = blk // core * wide
    first, parts = call(
        functools.partial(close_kernel, dim, ((shares, len(sums)), columns), place_of),
        rows + sums + kept,
        [((rhs, size), f32), ((members, rhs + 8, size), f32)],
        200 * 80 * points * size,
    )
    teams = [
        [(b * core + c) * grp + f * part + r for b in range(blk // core) for r in range(part)]
        for c in range(core)
        for f in range(far)
    ]
    parts = lax.all_to_all(parts, AXES, 0, 0, axis_index_groups=teams)
    return call(functools.partial(end_kernel, dim), [noise, packed, first, parts], [((rhs, size), f32)] * 3, 1)


def solution(mesh):
    in_specs = (P(None, AXES), P(), P(AXES), P(), P(None, AXES))
    out_specs = (P(None, AXES), P(None, AXES), P(None, AXES))
    blk, grp = mesh.shape["blk"], mesh.shape["grp"]

    def body(*arguments):
        return on_device(blk, grp, *arguments)

    return jax.shard_map(body, mesh=mesh, in_specs=in_specs, out_specs=out_specs, check_vma=False)
```
